32 devices in a mesh: dp: 1 (over z), ep: 32 (over y, x, core).
Axes of the slice: x: 4, y: 4, z: 1, core: 2. Of those that a mesh axis runs over, the one named last changes fastest.
The devices are a block of a 4x4x8 slice.
Arguments:
- x_in: bfloat16 [256, 2048], P(('dp', 'ep'))
- topk_idx: int32 [256, 8], P(('dp', 'ep'))
- topk_w: float32 [256, 8], P(('dp', 'ep'))
- w_up: bfloat16 [256, 2048, 512], P('ep')
- w_down: bfloat16 [256, 512, 2048], P('ep')
Outputs:
- output: bfloat16 [256, 2048], P(('dp', 'ep'))
All inputs are finite; a program needn't handle non-finite values.
Results may differ from the reference program's by a relative error of at most 0.00106.
Values are sent between devices in bfloat16 or wider.
A program may use at most 768 MiB of HBM per device.

```python
import jax
import jax.numpy as jnp
from jax import lax

TOK_DEV = 8
GROUP_SIZE = 32
D_MODEL = 2048
D_FF = 512
EXPERTS = 256
TOP_K = 8
TOKENS = TOK_DEV * GROUP_SIZE
PAIRS = TOKENS * TOP_K
ROW_WINDOW = min(64, TOKENS)


def draw_routing(route_key):
    key_perm, key_rank, key_start, key_roll = jax.random.split(route_key, 4)
    expert_order = jax.random.permutation(key_perm, EXPERTS).astype(jnp.int32)
    hot_pair = expert_order[:2]
    cold_cycle = expert_order[2:]
    cold_count = EXPERTS - 2
    ranks = jax.vmap(lambda one_key: jax.random.permutation(one_key, TOK_DEV))(jax.random.split(key_rank, GROUP_SIZE)).astype(jnp.int32)
    device_index = jnp.arange(GROUP_SIZE, dtype=jnp.int32)[:, None]
    cold_start = jax.random.randint(key_start, (), 0, cold_count, dtype=jnp.int32)
    cold_base = cold_start + (device_index * TOK_DEV + ranks) * (TOP_K - 1)
    cold_steps = jnp.arange(TOP_K - 1, dtype=jnp.int32)
    cold_ids = cold_cycle[(cold_base[:, :, None] + cold_steps) % cold_count]
    hot_ids = hot_pair[ranks % 2]
    picks = jnp.concatenate([hot_ids[:, :, None], cold_ids], axis=2).reshape(TOKENS, TOP_K)
    shifts = jax.random.randint(key_roll, (TOKENS, 1), 0, TOP_K, dtype=jnp.int32)
    slot_order = (jnp.arange(TOP_K, dtype=jnp.int32)[None, :] + shifts) % TOP_K
    return jnp.take_along_axis(picks, slot_order, axis=1)


def setup_inputs(seed: int = 0, part: int = 0) -> dict:
    part_key = jax.random.fold_in(jax.random.key(seed), part)
    key_x, key_route, key_gate = jax.random.split(part_key, 3)
    key_up, key_down = jax.random.split(jax.random.key(seed + 7919), 2)
    x_in = jax.random.normal(key_x, (TOKENS, D_MODEL), jnp.float32).astype(jnp.bfloat16)
    topk_idx = draw_routing(key_route)
    topk_w = jax.random.uniform(key_gate, (TOKENS, TOP_K), jnp.float32, 0.2, 1.0)
    w_up = lax.map(lambda one_key: (jax.random.normal(one_key, (D_MODEL, D_FF), jnp.float32) * D_MODEL ** -0.5).astype(jnp.bfloat16), jax.random.split(key_up, EXPERTS))
    w_down = lax.map(lambda one_key: (jax.random.normal(one_key, (D_FF, D_MODEL), jnp.float32) * D_FF ** -0.5).astype(jnp.bfloat16), jax.random.split(key_down, EXPERTS))
    return {'x_in': x_in, 'topk_idx': topk_idx, 'topk_w': topk_w, 'w_up': w_up, 'w_down': w_down}


def reference(x_in, topk_idx, topk_w, w_up, w_down):
    flat_ids = topk_idx.reshape(PAIRS)
    order = jnp.argsort(flat_ids, stable=True)
    pad_rows = jnp.zeros((ROW_WINDOW, D_MODEL), x_in.dtype)
    sorted_rows = jnp.concatenate([x_in[order // TOP_K], pad_rows], axis=0)
    counts = jnp.bincount(flat_ids, length=EXPERTS)
    starts = jnp.cumsum(counts) - counts

    def expert_step(expert, results):
        up_mat = w_up[expert]
        down_mat = w_down[expert]

        def window_step(window, acc_rows):
            base = starts[expert] + window * ROW_WINDOW
            rows = lax.dynamic_slice(sorted_rows, (base, 0), (ROW_WINDOW, D_MODEL))
            hidden = jax.nn.gelu(jnp.dot(rows, up_mat, preferred_element_type=jnp.float32), approximate=True).astype(jnp.bfloat16)
            result = jnp.dot(hidden, down_mat, preferred_element_type=jnp.float32).astype(jnp.bfloat16)
            valid = window * ROW_WINDOW + jnp.arange(ROW_WINDOW) < counts[expert]
            current = lax.dynamic_slice(acc_rows, (base, 0), (ROW_WINDOW, D_MODEL))
            return lax.dynamic_update_slice(acc_rows, jnp.where(valid[:, None], result, current), (base, 0))

        windows = (counts[expert] + ROW_WINDOW - 1) // ROW_WINDOW
        return lax.fori_loop(0, windows, window_step, results)

    results = jnp.zeros((PAIRS + ROW_WINDOW, D_MODEL), x_in.dtype)
    results = lax.fori_loop(0, EXPERTS, expert_step, results)
    pair_out = results[jnp.argsort(order)].reshape(TOKENS, TOP_K, D_MODEL)
    mixed = jnp.sum(topk_w[:, :, None] * pair_out.astype(jnp.float32), axis=1)
    return mixed.astype(jnp.bfloat16)
```

```python
import functools
import math

import jax
import jax.numpy as jnp
from jax import lax
from jax.experimental import pallas as pl
from jax.experimental.pallas import tpu as pltpu
from jax.sharding import PartitionSpec as P

MESH = pl.DeviceIdType.MESH
LANES = 128
KC = 4
QC = 4


def moe_kernel(side, x_hbm, ids_hbm, gates_hbm, up_hbm, down_hbm, y_ref,
               up, down, gath, meta, ids_v, gates_v, rows, z, h, gate, part, pair, ring, line, cross,
               in_sem, up_sem, down_sem,
               g1_s, g1_r, g2_s, g2_r, g3_s, g3_r,
               r0_s, r0_r, r1_s, r1_r, r2_s, r2_r):
    n_exp, dim, ff = up.shape
    tok = x_hbm.shape[0]
    total = 2 * side * side * tok
    kw = dim // KC
    qw = dim // QC
    me = lax.axis_index('ep')
    core = lax.rem(me, 2)
    col = lax.rem(me // 2, side)
    row = me // (2 * side)

    def at(dy, dx, dc=0):
        return {'ep': (lax.rem(row + dy, side) * side + lax.rem(col + dx, side)) * 2 + lax.rem(core + dc, 2)}

    def neg(d):
        return (side - d) % side

    def rcopy(src, dst, ss, rs, dev):
        return pltpu.make_async_remote_copy(src_ref=src, dst_ref=dst, send_sem=ss, recv_sem=rs, device_id=dev, device_id_type=MESH)

    loads = [pltpu.make_async_copy(x_hbm.at[:, pl.ds(k * kw, kw)], gath.at[k, 0, 0, 0], in_sem.at[k]) for k in range(KC)]
    loads.append(pltpu.make_async_copy(ids_hbm, ids_v, in_sem.at[KC]))
    loads.append(pltpu.make_async_copy(gates_hbm, gates_v, in_sem.at[KC + 1]))
    for c in loads:
        c.start()

    def up_copy(k, e):
        return pltpu.make_async_copy(up_hbm.at[e, pl.ds(k * kw, kw), :], up.at[e, pl.ds(k * kw, kw), :], up_sem.at[k, e])

    def down_copy(q, e):
        return pltpu.make_async_copy(down_hbm.at[e, :, pl.ds(q * qw, qw)], down.at[e, :, pl.ds(q * qw, qw)], down_sem.at[q, e])

    for k in range(KC):
        for e in range(n_exp):
            up_copy(k, e).start()
    for q in range(QC):
        for e in range(n_exp):
            down_copy(q, e).start()

    peers = [at(0, d) for d in range(1, side)] + [at(d, 0) for d in range(1, side)] + [at(0, 0, 1)]
    barrier = pltpu.get_barrier_semaphore()
    for dev in peers:
        pl.semaphore_signal(barrier, inc=1, device_id=dev, device_id_type=MESH)

    for c in loads[KC:]:
        c.wait()
    top = ids_v.shape[1]
    meta[0, 0, 0, 0] = jnp.full((tok, LANES), -1.0, jnp.float32)
    meta[0, 0, 0, 1] = jnp.zeros((tok, LANES), jnp.float32)
    meta[0, 0, 0, 0, :, 0:top] = ids_v[...].astype(jnp.float32)
    meta[0, 0, 0, 1, :, 0:top] = gates_v[...]
    for c in loads[:KC]:
        c.wait()
    pl.semaphore_wait(barrier, len(peers))

    def block(k):
        return meta if k == KC else gath.at[k]

    def first(k, d):
        b, lane = block(k), k % 2 == 0
        dst = b.at[0, 0, neg(d)] if lane else b.at[0, neg(d), 0]
        return rcopy(b.at[0, 0, 0], dst, g1_s.at[k, d], g1_r.at[k, neg(d)], at(0, d) if lane else at(d, 0))

    def first_in(k, d):
        b, lane = block(k), k % 2 == 0
        dst = b.at[0, 0, d] if lane else b.at[0, d, 0]
        return rcopy(b.at[0, 0, 0], dst, g1_s.at[k, d], g1_r.at[k, d], at(0, d) if lane else at(d, 0))

    def second(k, d):
        b, lane = block(k), k % 2 == 0
        src = b.at[0, 0] if lane else b.at[0, :, 0]
        dst = b.at[0, neg(d)] if lane else b.at[0, :, neg(d)]
        return rcopy(src, dst, g2_s.at[k, d], g2_r.at[k, neg(d)], at(d, 0) if lane else at(0, d))

    def second_in(k, d):
        b, lane = block(k), k % 2 == 0
        src = b.at[0, 0] if lane else b.at[0, :, 0]
        dst = b.at[0, d] if lane else b.at[0, :, d]
        return rcopy(src, dst, g2_s.at[k, d], g2_r.at[k, d], at(d, 0) if lane else at(0, d))

    def third(k):
        b = block(k)
        return rcopy(b.at[0], b.at[1], g3_s.at[k], g3_r.at[k], at(0, 0, 1))

    offs = [2, 1, 3] if side == 4 else list(range(1, side))
    streams = list(range(KC + 1))
    for k in streams:
        for d in offs:
            first(k, d).start()
    for k in streams:
        for d in offs:
            first_in(k, d).wait_recv()
        for d in offs:
            second(k, d).start()
    for k in streams:
        for d in offs:
            second_in(k, d).wait_recv()
        third(k).start()

    def wide(g, n):
        return jnp.concatenate([g] * (n // LANES), axis=1)

    for k in range(KC):
        third(k).wait_recv()
        rows[k] = gath[k].astype(jnp.float32).reshape(total, kw).astype(jnp.bfloat16)
        for e in range(n_exp):
            up_copy(k, e).wait()
        if k == KC - 1:
            third(KC).wait_recv()
            ids_all = meta[:, :, :, 0].reshape(total, LANES)
            gates_all = meta[:, :, :, 1].reshape(total, LANES)
            for e in range(n_exp):
                eid = (me * n_exp + e).astype(jnp.float32)
                g = jnp.sum(jnp.where(ids_all == eid, gates_all, 0.0), axis=1, keepdims=True)
                gate[e] = jnp.broadcast_to(g, (total, LANES))
        for e in range(n_exp):
            acc = jnp.dot(rows[k], up[e, pl.ds(k * kw, kw), :], preferred_element_type=jnp.float32)
            if k > 0:
                acc = z[e] + acc
            if k < KC - 1:
                z[e] = acc
            else:
                act = jax.nn.gelu(acc, approximate=True)
                h[e] = jnp.where(wide(gate[e], ff) > 0.0, act, 0.0).astype(jnp.bfloat16)

    def pair_out(q):
        return rcopy(part.at[q, 1], pair.at[q], r0_s.at[q], r0_r.at[q], at(0, 0, 1))

    def ring_out(q, d):
        lane = q % 2 == 0
        src = part.at[q, 0, :, d] if lane else part.at[q, 0, d]
        return rcopy(src, ring.at[q, neg(d)], r1_s.at[q, d], r1_r.at[q, neg(d)], at(0, d) if lane else at(d, 0))

    def ring_in(q, d):
        lane = q % 2 == 0
        src = part.at[q, 0, :, d] if lane else part.at[q, 0, d]
        return rcopy(src, ring.at[q, d], r1_s.at[q, d], r1_r.at[q, d], at(0, d) if lane else at(d, 0))

    def cross_out(q, d):
        lane = q % 2 == 0
        return rcopy(line.at[q, d], cross.at[q, neg(d)], r2_s.at[q, d], r2_r.at[q, neg(d)], at(d, 0) if lane else at(0, d))

    def cross_in(q, d):
        lane = q % 2 == 0
        return rcopy(line.at[q, d], cross.at[q, d], r2_s.at[q, d], r2_r.at[q, d], at(d, 0) if lane else at(0, d))

    def stage1(q):
        pair_out(q).wait_recv()
        part[q, 0] = part[q, 0] + pair[q]
        for d in offs:
            ring_out(q, d).start()

    def stage2(q):
        for d in offs:
            ring_in(q, d).wait_recv()
        own = part[q, 0, :, 0] if q % 2 == 0 else part[q, 0, 0]
        for d in range(1, side):
            own = own + ring[q, d]
        line[q] = own
        for d in offs:
            cross_out(q, d).start()

    def stage3(q):
        for d in offs:
            cross_in(q, d).wait_recv()
        s = line[q, 0]
        for d in range(1, side):
            s = s + cross[q, d]
        y_ref[:, q * qw:(q + 1) * qw] = s.astype(y_ref.dtype)

    for q in range(QC):
        for e in range(n_exp):
            down_copy(q, e).wait()
        for e in range(n_exp):
            o = jnp.dot(h[e], down[e, :, pl.ds(q * qw, qw)], preferred_element_type=jnp.float32)
            o = o.astype(jnp.bfloat16).astype(jnp.float32) * wide(gate[e], qw)
            o = o.reshape(2, side, side, tok, qw)
            part[q] = o if e == 0 else part[q] + o
        pair_out(q).start()
        if q >= 1:
            stage1(q - 1)
        if q >= 3:
            stage2(q - 3)
    stage1(QC - 1)
    for q in range(QC):
        if q >= QC - 3:
            stage2(q)
    for q in range(QC):
        stage3(q)

    for k in streams:
        for d in offs:
            first(k, d).wait_send()
            second(k, d).wait_send()
        third(k).wait_send()
    for q in range(QC):
        pair_out(q).wait_send()
        for d in offs:
            ring_out(q, d).wait_send()
            cross_out(q, d).wait_send()


def solution(mesh):
    group = mesh.shape['ep']
    side = math.isqrt(group // 2)
    token_spec = P(('dp', 'ep'), None)
    expert_spec = P('ep', None, None)

    def local_layer(x_loc, ids_loc, gates_loc, w_up, w_down):
        tok, dim = x_loc.shape
        n_exp, _, ff = w_up.shape
        total = tok * group
        kw, qw = dim // KC, dim // QC
        f32, bf16 = jnp.float32, jnp.bfloat16
        dma = pltpu.SemaphoreType.DMA
        scratch = [
            pltpu.VMEM(w_up.shape, bf16),
            pltpu.VMEM(w_down.shape, bf16),
            pltpu.VMEM((KC, 2, side, side, tok, kw), bf16),
            pltpu.VMEM((2, side, side, 2, tok, LANES), f32),
            pltpu.VMEM(ids_loc.shape, jnp.int32),
            pltpu.VMEM(gates_loc.shape, f32),
            pltpu.VMEM((KC, total, kw), bf16),
            pltpu.VMEM((n_exp, total, ff), f32),
            pltpu.VMEM((n_exp, total, ff), bf16),
            pltpu.VMEM((n_exp, total, LANES), f32),
            pltpu.VMEM((QC, 2, side, side, tok, qw), f32),
            pltpu.VMEM((QC, side, side, tok, qw), f32),
            pltpu.VMEM((QC, side, side, tok, qw), f32),
            pltpu.VMEM((QC, side, tok, qw), f32),
            pltpu.VMEM((QC, side, tok, qw), f32),
            dma((KC + 2,)), dma((KC, n_exp)), dma((QC, n_exp)),
            dma((KC + 1, side)), dma((KC + 1, side)), dma((KC + 1, side)), dma((KC + 1, side)), dma((KC + 1,)), dma((KC + 1,)),
            dma((QC,)), dma((QC,)), dma((QC, side)), dma((QC, side)), dma((QC, side)), dma((QC, side)),
        ]
        return pl.pallas_call(
            functools.partial(moe_kernel, side),
            out_shape=jax.ShapeDtypeStruct((tok, dim), bf16),
            in_specs=[pl.BlockSpec(memory_space=pl.ANY)] * 5,
            out_specs=pl.BlockSpec(memory_space=pltpu.VMEM),
            scratch_shapes=scratch,
            compiler_params=pltpu.CompilerParams(collective_id=0, has_side_effects=True, vmem_limit_bytes=60 * 1024 * 1024),
        )(x_loc, ids_loc, gates_loc, w_up, w_down)

    return jax.shard_map(local_layer, mesh=mesh, in_specs=(token_spec, token_spec, token_spec, expert_spec, expert_spec), out_specs=token_spec, check_vma=False)
```

```python
import functools
import math

import jax
import jax.numpy as jnp
from jax import lax
from jax.experimental import pallas as pl
from jax.experimental.pallas import tpu as pltpu
from jax.sharding import PartitionSpec as P

MESH = pl.DeviceIdType.MESH
LANES = 128
KC = 4
QC = 4
LAG = 2


def wide(g, n):
    return jnp.concatenate([g] * (n // LANES), axis=1)


def moe_kernel(side, x_hbm, ids_hbm, gates_hbm, up_hbm, down_hbm, y_ref,
               up, down, gath, meta, ids_v, gates_v, rows, z, h, gate, part, pair, ring, line, cross,
               in_sem, up_sem, down_sem, go, ag_s, ag_r, fw_s, fw_r, pair_s, pair_r, ring_s, ring_r, cross_s, cross_r):
    n_exp, dim, ff = up.shape
    tok = x_hbm.shape[0]
    chips = side * side
    half = chips * tok
    kw = dim // KC
    qw = dim // QC
    me = lax.axis_index('ep')
    core = lax.rem(me, 2)
    col = lax.rem(me // 2, side)
    row = me // (2 * side)

    def at(dy, dx, dc=0):
        return {'ep': (lax.rem(row + dy, side) * side + lax.rem(col + dx, side)) * 2 + lax.rem(core + dc, 2)}

    def neg(d):
        return (side - d) % side

    def rcopy(src, dst, ss, rs, dev):
        return pltpu.make_async_remote_copy(src_ref=src, dst_ref=dst, send_sem=ss, recv_sem=rs, device_id=dev, device_id_type=MESH)

    partner = at(0, 0, 1)
    offs = [(dy, dx) for dy in range(side) for dx in range(side) if dy or dx]
    offs.sort(key=lambda o: -(min(o[0], side - o[0]) + min(o[1], side - o[1])))
    line_offs = sorted(range(1, side), key=lambda d: -min(d, side - d))

    x_loads = [pltpu.make_async_copy(x_hbm.at[:, pl.ds(k * kw, kw)], gath.at[k, core, 0], in_sem.at[0]) for k in range(KC)]
    loads = [pltpu.make_async_copy(ids_hbm, ids_v, in_sem.at[1]), pltpu.make_async_copy(gates_hbm, gates_v, in_sem.at[2])]
    for c in loads + x_loads:
        c.start()
    barrier = pltpu.get_barrier_semaphore()
    for dy, dx in offs:
        pl.semaphore_signal(barrier, inc=1, device_id=at(dy, dx), device_id_type=MESH)
    pl.semaphore_signal(barrier, inc=1, device_id=partner, device_id_type=MESH)
    for c in loads:
        c.wait()
    top = ids_v.shape[1]
    meta[core, 0] = jnp.full((tok, LANES), -1.0, jnp.float32)
    meta[core, 0, :, 0:top] = ids_v[...].astype(jnp.float32)
    meta[core, 0, :, LANES // 2:LANES // 2 + top] = gates_v[...]
    pltpu.make_async_copy(gath.at[:, core, 0], gath.at[:, core, 0], in_sem.at[0]).wait()

    def up_copy(k):
        return pltpu.make_async_copy(up_hbm.at[:, pl.ds(k * kw, kw), :], up.at[:, pl.ds(k * kw, kw), :], up_sem.at[k])

    def down_copy(q):
        return pltpu.make_async_copy(down_hbm.at[:, :, pl.ds(q * qw, qw)], down.at[:, :, pl.ds(q * qw, qw)], down_sem.at[q])

    for k in range(KC):
        up_copy(k).start()
    for q in range(QC):
        down_copy(q).start()
    pl.semaphore_wait(barrier, len(offs) + 1)

    def block(k):
        return meta if k == KC else gath.at[k]

    def send(k, o):
        b = block(k)
        return rcopy(b.at[core, 0], b.at[core, neg(o[0]) * side + neg(o[1])], ag_s.at[k], ag_r.at[k], at(*o))

    def gathered(k):
        b = block(k).at[core, pl.ds(1, chips - 1)]
        return rcopy(b, b, ag_s.at[k], ag_r.at[k], partner)

    def forward(k):
        b = block(k).at[core]
        return rcopy(b, b, fw_s.at[k], fw_r.at[k], partner)

    def forwarded(k):
        b = block(k).at[1 - core]
        return rcopy(b, b, fw_s.at[k], fw_r.at[k], partner)

    streams = [KC] + list(range(KC))

    @pl.when(core == 1)
    def _():
        pl.semaphore_wait(go, 1)

    for k in streams:
        for o in offs:
            send(k, o).start()

    @pl.when(core == 0)
    def _():
        for k in streams[:-1]:
            gathered(k).wait_send()
        pl.semaphore_signal(go, inc=1, device_id=partner, device_id_type=MESH)
        gathered(streams[-1]).wait_send()

    def pass_on(k):
        gathered(k).wait_recv()
        forward(k).start()

    def arrive(c, k):
        if c == 0:
            @pl.when(core == 0)
            def _():
                pass_on(k)

        @pl.when(core != c)
        def _():
            forwarded(k).wait_recv()

    def find_gates(c):
        ids_all = meta[c].reshape(half, LANES)
        gates_all = pltpu.roll(ids_all, LANES // 2, axis=1)
        lane = lax.broadcasted_iota(jnp.int32, (half, LANES), 1)
        for e in range(n_exp):
            eid = (me * n_exp + e).astype(jnp.float32)
            g = jnp.sum(jnp.where((ids_all == eid) & (lane < top), gates_all, 0.0), axis=1, keepdims=True)
            gate[c, e] = jnp.broadcast_to(g, (half, LANES))

    def up_chunk(c, k):
        rows[k] = gath[k, c].astype(jnp.float32).reshape(half, kw).astype(jnp.bfloat16)
        for e in range(n_exp):
            acc = jnp.dot(rows[k], up[e, pl.ds(k * kw, kw), :], preferred_element_type=jnp.float32)
            if k > 0:
                acc = z[e] + acc
            if k < KC - 1:
                z[e] = acc
            else:
                act = jax.nn.gelu(acc, approximate=True)
                h[e] = jnp.where(wide(gate[c, e], ff) > 0.0, act, 0.0).astype(jnp.bfloat16)

    def down_chunk(c, q):
        for e in range(n_exp):
            o = jnp.dot(h[e], down[e, :, pl.ds(q * qw, qw)], preferred_element_type=jnp.float32)
            o = o.astype(jnp.bfloat16).astype(jnp.float32) * wide(gate[c, e], qw)
            o = o.reshape(side, side, tok, qw)
            part[c, q] = o if e == 0 else part[c, q] + o

    def pair_out(c, q):
        return rcopy(part.at[c, q], pair.at[q], pair_s, pair_r.at[q], partner)

    def ring_out(c, q, d):
        lane = q % 2 == 0
        src = part.at[c, q, :, d] if lane else part.at[c, q, d]
        return rcopy(src, ring.at[q, neg(d)], ring_s, ring_r.at[q], at(0, d) if lane else at(d, 0))

    def cross_out(q, d):
        lane = q % 2 == 0
        return rcopy(line.at[q, d], cross.at[q, neg(d)], cross_s, cross_r.at[q], at(d, 0) if lane else at(0, d))

    def came(ref, ss, rs):
        return rcopy(ref, ref, ss, rs, partner)

    def stage1(c, q):
        came(pair.at[q], pair_s, pair_r.at[q]).wait_recv()
        part[c, q] = part[c, q] + pair[q]
        for d in line_offs:
            ring_out(c, q, d).start()

    def stage2(c, q):
        came(ring.at[q, pl.ds(1, side - 1)], ring_s, ring_r.at[q]).wait_recv()
        own = part[c, q, :, 0] if q % 2 == 0 else part[c, q, 0]
        for d in range(1, side):
            own = own + ring[q, d]
        line[q] = own
        for d in line_offs:
            cross_out(q, d).start()

    def stage3(q):
        came(cross.at[q, pl.ds(1, side - 1)], cross_s, cross_r.at[q]).wait_recv()
        s = line[q, 0]
        for d in range(1, side):
            s = s + cross[q, d]
        y_ref[:, q * qw:(q + 1) * qw] = s.astype(y_ref.dtype)

    arrive(0, KC)
    find_gates(0)
    for k in range(KC):
        arrive(0, k)
        up_copy(k).wait()
        up_chunk(0, k)
    pending = list(streams)

    def next_pass(n):
        ks, pending[:] = pending[:n], pending[n:]
        for k in ks:
            pass_on(k)

    @pl.when(core == 1)
    def _():
        next_pass(2)
    for q in range(QC):
        down_copy(q).wait()
        down_chunk(0, q)

        @pl.when(core == 1)
        def _():
            pair_out(0, q).start()
            next_pass(1 if q < QC - 1 else len(pending))

    arrive(1, KC)
    find_gates(1)
    for k in range(KC):
        arrive(1, k)
        up_chunk(1, k)
        if k < QC:
            @pl.when(core == 0)
            def _():
                stage1(0, k)
    for q in range(QC):
        down_chunk(1, q)

        @pl.when(core == 0)
        def _():
            pair_out(1, q).start()
            if q >= 1:
                stage2(0, q - 1)

        @pl.when(core == 1)
        def _():
            if q >= LAG:
                stage1(1, q - LAG)

    @pl.when(core == 0)
    def _():
        stage2(0, QC - 1)

    @pl.when(core == 1)
    def _():
        for q in range(QC - LAG, QC):
            stage1(1, q)
        for q in range(QC):
            stage2(1, q)
    for q in range(QC):
        stage3(q)

    @pl.when(core == 1)
    def _():
        for k in streams:
            gathered(k).wait_send()
    for k in streams:
        forward(k).wait_send()
    came(pair, pair_s, pair_r.at[0]).wait_send()
    came(ring.at[:, pl.ds(1, side - 1)], ring_s, ring_r.at[0]).wait_send()
    came(cross.at[:, pl.ds(1, side - 1)], cross_s, cross_r.at[0]).wait_send()


def solution(mesh):
    group = mesh.shape['ep']
    side = math.isqrt(group // 2)
    token_spec = P(('dp', 'ep'), None)
    expert_spec = P('ep', None, None)

    def local_layer(x_loc, ids_loc, gates_loc, w_up, w_down):
        tok, dim = x_loc.shape
        n_exp, _, ff = w_up.shape
        half = tok * group // 2
        kw, qw = dim // KC, dim // QC
        f32, bf16 = jnp.float32, jnp.bfloat16
        dma = pltpu.SemaphoreType.DMA
        scratch = [
            pltpu.VMEM(w_up.shape, bf16),
            pltpu.VMEM(w_down.shape, bf16),
            pltpu.VMEM((KC, 2, side * side, tok, kw), bf16),
            pltpu.VMEM((2, side * side, tok, LANES), f32),
            pltpu.VMEM(ids_loc.shape, jnp.int32),
            pltpu.VMEM(gates_loc.shape, f32),
            pltpu.VMEM((KC, half, kw), bf16),
            pltpu.VMEM((n_exp, half, ff), f32),
            pltpu.VMEM((n_exp, half, ff), bf16),
            pltpu.VMEM((2, n_exp, half, LANES), f32),
            pltpu.VMEM((2, QC, side, side, tok, qw), f32),
            pltpu.VMEM((QC, side, side, tok, qw), f32),
            pltpu.VMEM((QC, side, side, tok, qw), f32),
            pltpu.VMEM((QC, side, tok, qw), f32),
            pltpu.VMEM((QC, side, tok, qw), f32),
            dma((3,)), dma((KC,)), dma((QC,)), pltpu.SemaphoreType.REGULAR,
            dma((KC + 1,)), dma((KC + 1,)), dma((KC + 1,)), dma((KC + 1,)),
            dma, dma((QC,)), dma, dma((QC,)), dma, dma((QC,)),
        ]
        return pl.pallas_call(
            functools.partial(moe_kernel, side),
            out_shape=jax.ShapeDtypeStruct((tok, dim), bf16),
            in_specs=[pl.BlockSpec(memory_space=pl.ANY)] * 5,
            out_specs=pl.BlockSpec(memory_space=pltpu.VMEM),
            scratch_shapes=scratch,
            compiler_params=pltpu.CompilerParams(collective_id=0, has_side_effects=True, vmem_limit_bytes=60 * 1024 * 1024),
        )(x_loc, ids_loc, gates_loc, w_up, w_down)

    return jax.shard_map(local_layer, mesh=mesh, in_specs=(token_spec, token_spec, token_spec, expert_spec, expert_spec), out_specs=token_spec, check_vma=False)
```

```python
import functools
import math

import jax
import jax.numpy as jnp
from jax import lax
from jax.experimental import pallas as pl
from jax.experimental.pallas import tpu as pltpu
from jax.sharding import PartitionSpec as P

MESH = pl.DeviceIdType.MESH
LANES = 128
KC = 4
GO = 4
QC = 4
PASS = ((0, 1), (2,), (3,), (4,))
BLOCKS = (((0,), (1,), (2,), (3,)), ((0,), (1,), (2,), (3,)))
FLAT = True


def wide(g, n):
    return jnp.concatenate([g] * (n // LANES), axis=1)


def gelu(v):
    a = math.sqrt(2 / math.pi)
    half_v = 0.5 * v
    return half_v + half_v * jnp.tanh(v * (a + (a * 0.044715) * (v * v)))


def moe_kernel(side, x_hbm, ids_hbm, gates_hbm, up_hbm, down_hbm, y_ref,
               up, down, gath, meta, ids_v, gates_v, rows, z, h, gate, part, pair, ring, line, cross, flat,
               in_sem, up_sem, down_sem, go, ag_s, ag_r, fw_s, fw_r, pair_s, pair_r, ring_s, ring_r, cross_s, cross_r, flat_s, flat_r):
    n_exp, dim, ff = up.shape
    tok = x_hbm.shape[0]
    chips = side * side
    half = chips * tok
    kw = dim // KC
    qw = dim // QC
    me = lax.axis_index('ep')
    core = lax.rem(me, 2)
    col = lax.rem(me // 2, side)
    row = me // (2 * side)

    def at(dy, dx, dc=0):
        return {'ep': (lax.rem(row + dy, side) * side + lax.rem(col + dx, side)) * 2 + lax.rem(core + dc, 2)}

    def neg(d):
        return (side - d) % side

    def rcopy(src, dst, ss, rs, dev):
        return pltpu.make_async_remote_copy(src_ref=src, dst_ref=dst, send_sem=ss, recv_sem=rs, device_id=dev, device_id_type=MESH)

    partner = at(0, 0, 1)
    offs = [(dy, dx) for dy in range(side) for dx in range(side) if dy or dx]
    offs.sort(key=lambda o: -(min(o[0], side - o[0]) + min(o[1], side - o[1])))
    line_offs = sorted(range(1, side), key=lambda d: -min(d, side - d))

    x_loads = [pltpu.make_async_copy(x_hbm.at[:, pl.ds(k * kw, kw)], gath.at[k, core, 0], in_sem.at[0]) for k in range(KC)]
    loads = [pltpu.make_async_copy(ids_hbm, ids_v, in_sem.at[1]), pltpu.make_async_copy(gates_hbm, gates_v, in_sem.at[2])]
    for c in x_loads + loads:
        c.start()
    barrier = pltpu.get_barrier_semaphore()
    for dy, dx in offs:
        pl.semaphore_signal(barrier, inc=1, device_id=at(dy, dx), device_id_type=MESH)
    pl.semaphore_signal(barrier, inc=1, device_id=partner, device_id_type=MESH)
    for c in loads:
        c.wait()
    top = ids_v.shape[1]
    meta[core, 0] = jnp.full((tok, LANES), -1.0, jnp.float32)
    meta[core, 0, :, 0:top] = ids_v[...].astype(jnp.float32)
    meta[core, 0, :, LANES // 2:LANES // 2 + top] = gates_v[...]
    pltpu.make_async_copy(gath.at[:, core, 0], gath.at[:, core, 0], in_sem.at[0]).wait()

    def up_copy(k):
        s = pl.ds(k * kw, kw)
        return pltpu.make_async_copy(up_hbm.at[:, s], up.at[:, s], up_sem.at[k])

    def up_wait(k):
        up_copy(k).wait()

    def down_copy(q):
        return pltpu.make_async_copy(down_hbm.at[:, :, pl.ds(q * qw, qw)], down.at[:, :, pl.ds(q * qw, qw)], down_sem.at[q])

    for k in range(KC):
        up_copy(k).start()
    for q in range(QC):
        down_copy(q).start()
    pl.semaphore_wait(barrier, len(offs) + 1)

    block = [meta] + [gath.at[k] for k in range(KC)]
    streams = range(KC + 1)

    def send(k, o):
        b = block[k]
        return rcopy(b.at[core, 0], b.at[core, neg(o[0]) * side + neg(o[1])], ag_s.at[k], ag_r.at[k], at(*o))

    def gathered(k):
        b = block[k].at[core, pl.ds(1, chips - 1)]
        return rcopy(b, b, ag_s.at[k], ag_r.at[k], partner)

    def forward(k):
        b = block[k].at[core]
        return rcopy(b, b, fw_s.at[k], fw_r.at[k], partner)

    def forwarded(k):
        b = block[k].at[1 - core]
        return rcopy(b, b, fw_s.at[k], fw_r.at[k], partner)

    @pl.when(core == 1)
    def _():
        pl.semaphore_wait(go, 1)

    for k in streams:
        for o in offs:
            send(k, o).start()

    @pl.when(core == 0)
    def _():
        for k in range(GO):
            gathered(k).wait_send()
        pl.semaphore_signal(go, inc=1, device_id=partner, device_id_type=MESH)

    def pass_on(k):
        gathered(k).wait_recv()
        forward(k).start()

    def arrive(c, k):
        if c == 0:
            @pl.when(core == 0)
            def _():
                pass_on(k)

        @pl.when(core != c)
        def _():
            forwarded(k).wait_recv()

    def find_gates(c):
        ids_all = meta[c].reshape(half, LANES)
        gates_all = pltpu.roll(ids_all, LANES // 2, axis=1)
        lane = lax.broadcasted_iota(jnp.int32, (half, LANES), 1)
        for e in range(n_exp):
            eid = (me * n_exp + e).astype(jnp.float32)
            g = jnp.sum(jnp.where((ids_all == eid) & (lane < top), gates_all, 0.0), axis=1, keepdims=True)
            gate[c, e] = jnp.broadcast_to(g, (half, LANES))

    def up_chunk(c, k):
        if k == 0:
            find_gates(c)
        rows[k] = gath[k, c].astype(jnp.float32).reshape(half, kw).astype(jnp.bfloat16)
        for e in range(n_exp):
            acc = jnp.dot(rows[k], up[e, pl.ds(k * kw, kw), :], preferred_element_type=jnp.float32)
            if k > 0:
                acc = z[e] + acc
            if k < KC - 1:
                z[e] = acc
            else:
                act = gelu(acc)
                h[e] = jnp.where(wide(gate[c, e], ff) > 0.0, act, 0.0).astype(jnp.bfloat16)

    def down_chunk(c, q):
        for e in range(n_exp):
            o = jnp.dot(h[e], down[e, :, pl.ds(q * qw, qw)], preferred_element_type=jnp.float32)
            o = o.astype(jnp.bfloat16).astype(jnp.float32) * wide(gate[c, e], qw)
            o = o.reshape(side, side, tok, qw)
            part[c, q] = o if e == 0 else part[c, q] + o

    def pair_out(c, qs):
        r = pl.ds(qs[0], len(qs))
        return rcopy(part.at[c, r], pair.at[r], pair_s, pair_r.at[qs[0]], partner)

    def ring_out(c, q, d):
        lane = q % 2 == 0
        src = part.at[c, q, :, d] if lane else part.at[c, q, d]
        return rcopy(src, ring.at[q, neg(d)], ring_s, ring_r.at[q], at(0, d) if lane else at(d, 0))

    def cross_out(q, d):
        lane = q % 2 == 0
        return rcopy(line.at[q, d], cross.at[q, neg(d)], cross_s, cross_r.at[q], at(d, 0) if lane else at(0, d))

    def came(ref, ss, rs):
        return rcopy(ref, ref, ss, rs, partner)

    def stage1(c, qs):
        came(pair.at[pl.ds(qs[0], len(qs))], pair_s, pair_r.at[qs[0]]).wait_recv()
        for q in qs:
            part[c, q] = part[c, q] + pair[q]
        for q in qs:
            if c == 1 and q in direct:
                for o in offs:
                    i, j = neg(o[0]), neg(o[1])
                    rcopy(part.at[c, q, o[0], o[1]], flat.at[i * side + j], flat_s, flat_r, at(*o)).start()
            else:
                for d in line_offs:
                    ring_out(c, q, d).start()

    def stage2(c, q):
        came(ring.at[q, pl.ds(1, side - 1)], ring_s, ring_r.at[q]).wait_recv()
        own = part[c, q, :, 0] if q % 2 == 0 else part[c, q, 0]
        for d in range(1, side):
            own = own + ring[q, d]
        line[q] = own
        for d in line_offs:
            cross_out(q, d).start()

    def stage3(q):
        came(cross.at[q, pl.ds(1, side - 1)], cross_s, cross_r.at[q]).wait_recv()
        t = line[q, 0]
        for d in range(1, side):
            t = t + cross[q, d]
        y_ref[:, q * qw:(q + 1) * qw] = t.astype(y_ref.dtype)

    def stage_flat(q):
        came(flat.at[pl.ds(1, chips - 1)], flat_s, flat_r).wait_recv()
        t = part[1, q, 0, 0]
        for j in range(1, chips):
            t = t + flat[j]
        y_ref[:, q * qw:(q + 1) * qw] = t.astype(y_ref.dtype)

    direct = (QC - 1,) if FLAT else ()
    rest = [q for q in range(QC) if q not in direct]

    arrive(0, 0)
    for k in range(KC):
        arrive(0, k + 1)
        up_wait(k)
        up_chunk(0, k)
    for i, qs in enumerate(BLOCKS[0]):
        @pl.when(core == 1)
        def _():
            for k in PASS[i]:
                pass_on(k)
        for q in qs:
            down_copy(q).wait()
        for q in qs:
            down_chunk(0, q)

        @pl.when(core == 1)
        def _():
            pair_out(0, qs).start()

    arrive(1, 0)
    for k in range(KC):
        arrive(1, k + 1)
        up_chunk(1, k)
        if True:
            @pl.when(core == 0)
            def _():
                stage1(0, BLOCKS[0][k])
    for i, qs in enumerate(BLOCKS[1]):
        for q in qs:
            down_chunk(1, q)

        @pl.when(core == 0)
        def _():
            pair_out(1, qs).start()

        @pl.when(core == 1)
        def _():
            stage1(1, qs)

    @pl.when(core == 0)
    def _():
        for q in range(QC):
            stage2(0, q)
        for q in range(QC):
            stage3(q)

    @pl.when(core == 1)
    def _():
        for q in rest:
            stage2(1, q)
        for q in direct:
            stage_flat(q)
        for q in rest:
            stage3(q)
        for k in range(GO):
            gathered(k).wait_send()

    for k in range(GO, KC + 1):
        gathered(k).wait_send()
    for k in streams:
        forward(k).wait_send()

    @pl.when(core == 0)
    def _():
        came(pair, pair_s, pair_r.at[0]).wait_send()
        came(ring.at[:, pl.ds(1, side - 1)], ring_s, ring_r.at[0]).wait_send()
        came(cross.at[:, pl.ds(1, side - 1)], cross_s, cross_r.at[0]).wait_send()

    @pl.when(core == 1)
    def _():
        n = len(rest)
        came(pair, pair_s, pair_r.at[0]).wait_send()
        came(ring.at[pl.ds(0, n), pl.ds(1, side - 1)], ring_s, ring_r.at[0]).wait_send()
        came(cross.at[pl.ds(0, n), pl.ds(1, side - 1)], cross_s, cross_r.at[0]).wait_send()
        if direct:
            came(flat.at[pl.ds(1, chips - 1)], flat_s, flat_r).wait_send()


def solution(mesh):
    group = mesh.shape['ep']
    side = math.isqrt(group // 2)
    token_spec = P(('dp', 'ep'), None)
    expert_spec = P('ep', None, None)

    def local_layer(x_loc, ids_loc, gates_loc, w_up, w_down):
        tok, dim = x_loc.shape
        n_exp, _, ff = w_up.shape
        half = tok * group // 2
        qw = dim // QC
        f32, bf16 = jnp.float32, jnp.bfloat16
        dma = pltpu.SemaphoreType.DMA
        scratch = [
            pltpu.VMEM(w_up.shape, bf16),
            pltpu.VMEM(w_down.shape, bf16),
            pltpu.VMEM((KC, 2, side * side, tok, dim // KC), bf16),
            pltpu.VMEM((2, side * side, tok, LANES), f32),
            pltpu.VMEM(ids_loc.shape, jnp.int32),
            pltpu.VMEM(gates_loc.shape, f32),
            pltpu.VMEM((KC, half, dim // KC), bf16),
            pltpu.VMEM((n_exp, half, ff), f32),
            pltpu.VMEM((n_exp, half, ff), bf16),
            pltpu.VMEM((2, n_exp, half, LANES), f32),
            pltpu.VMEM((2, QC, side, side, tok, qw), f32),
            pltpu.VMEM((QC, side, side, tok, qw), f32),
            pltpu.VMEM((QC, side, side, tok, qw), f32),
            pltpu.VMEM((QC, side, tok, qw), f32),
            pltpu.VMEM((QC, side, tok, qw), f32),
            pltpu.VMEM((side * side, tok, qw), f32),
            dma((3,)), dma((KC,)), dma((QC,)), pltpu.SemaphoreType.REGULAR,
            dma((KC + 1,)), dma((KC + 1,)), dma((KC + 1,)), dma((KC + 1,)),
            dma, dma((QC,)), dma, dma((QC,)), dma, dma((QC,)), dma, dma,
        ]
        return pl.pallas_call(
            functools.partial(moe_kernel, side),
            out_shape=pltpu.VMEM((tok, dim), bf16),
            in_specs=[pl.BlockSpec(memory_space=pl.ANY)] * 5,
            out_specs=pl.BlockSpec(memory_space=pltpu.VMEM),
            scratch_shapes=scratch,
            compiler_params=pltpu.CompilerParams(collective_id=0, has_side_effects=True, vmem_limit_bytes=60 * 1024 * 1024),
        )(x_loc, ids_loc, gates_loc, w_up, w_down)

    return jax.shard_map(local_layer, mesh=mesh, in_specs=(token_spec, token_spec, token_spec, expert_spec, expert_spec), out_specs=token_spec, check_vma=False)
```

```python
import functools
import math

import jax
import jax.numpy as jnp
from jax import lax
from jax.experimental import pallas as pl
from jax.experimental.pallas import tpu as pltpu
from jax.sharding import PartitionSpec as P

MESH = pl.DeviceIdType.MESH
LANES = 128
KC = 4
GO = 4
QC = 4
PASS = ((0, 1), (2,), (3,), (4,))
BLOCKS = (((0,), (1,), (2,), (3,)), ((0,), (1,), (2,), (3,)))
FLAT = True


def wide(g, n):
    return jnp.concatenate([g] * (n // LANES), axis=1)


def gelu(v):
    a = math.sqrt(2 / math.pi)
    half_v = 0.5 * v
    return half_v + half_v * jnp.tanh(v * (a + (a * 0.044715) * (v * v)))


def moe_kernel(side, x_hbm, ids_hbm, gates_hbm, up_hbm, down_hbm, y_ref,
               up, down, gath, meta, ids_v, gates_v, rows, z, h, gate, part, pair, ring, line, cross, flat,
               in_sem, up_sem, down_sem, go, ag_s, ag_r, fw_s, fw_r, pair_s, pair_r, ring_s, ring_r, cross_s, cross_r, flat_s, flat_r):
    n_exp, dim, ff = up.shape
    tok = x_hbm.shape[0]
    chips = side * side
    half = chips * tok
    kw = dim // KC
    qw = dim // QC
    me = lax.axis_index('ep')
    core = lax.rem(me, 2)
    col = lax.rem(me // 2, side)
    row = me // (2 * side)

    def at(dy, dx, dc=0):
        return {'ep': (lax.rem(row + dy, side) * side + lax.rem(col + dx, side)) * 2 + lax.rem(core + dc, 2)}

    def neg(d):
        return (side - d) % side

    def rcopy(src, dst, ss, rs, dev):
        return pltpu.make_async_remote_copy(src_ref=src, dst_ref=dst, send_sem=ss, recv_sem=rs, device_id=dev, device_id_type=MESH)

    partner = at(0, 0, 1)
    offs = [(dy, dx) for dy in range(side) for dx in range(side) if dy or dx]
    offs.sort(key=lambda o: -(min(o[0], side - o[0]) + min(o[1], side - o[1])))
    line_offs = sorted(range(1, side), key=lambda d: -min(d, side - d))

    x_loads = [pltpu.make_async_copy(x_hbm.at[:, pl.ds(k * kw, kw)], gath.at[k, core, 0], in_sem.at[0]) for k in range(KC)]
    loads = [pltpu.make_async_copy(ids_hbm, ids_v, in_sem.at[1]), pltpu.make_async_copy(gates_hbm, gates_v, in_sem.at[2])]
    for c in x_loads + loads:
        c.start()
    barrier = pltpu.get_barrier_semaphore()
    for dy, dx in offs:
        pl.semaphore_signal(barrier, inc=1, device_id=at(dy, dx), device_id_type=MESH)
    pl.semaphore_signal(barrier, inc=1, device_id=partner, device_id_type=MESH)
    for c in loads:
        c.wait()
    top = ids_v.shape[1]
    meta[core, 0] = jnp.full((tok, LANES), -1.0, jnp.float32)
    meta[core, 0, :, 0:top] = ids_v[...].astype(jnp.float32)
    meta[core, 0, :, LANES // 2:LANES // 2 + top] = gates_v[...]
    pltpu.make_async_copy(gath.at[:, core, 0], gath.at[:, core, 0], in_sem.at[0]).wait()

    def up_copy(k):
        s = pl.ds(k * kw, kw)
        return pltpu.make_async_copy(up_hbm.at[:, s], up.at[:, s], up_sem)

    def up_wait(k):
        if k == 0:
            pltpu.make_async_copy(up_hbm, up, up_sem).wait()

    def down_copy(q):
        return pltpu.make_async_copy(down_hbm.at[:, :, pl.ds(q * qw, qw)], down.at[:, :, pl.ds(q * qw, qw)], down_sem.at[q])

    for k in range(KC):
        up_copy(k).start()
    for q in range(QC):
        down_copy(q).start()
    pl.semaphore_wait(barrier, len(offs) + 1)

    block = [meta] + [gath.at[k] for k in range(KC)]
    streams = range(KC + 1)

    def send(k, o):
        b = block[k]
        return rcopy(b.at[core, 0], b.at[core, neg(o[0]) * side + neg(o[1])], ag_s.at[k], ag_r.at[k], at(*o))

    def gathered(k):
        b = block[k].at[core, pl.ds(1, chips - 1)]
        return rcopy(b, b, ag_s.at[k], ag_r.at[k], partner)

    def forward(k):
        b = block[k].at[core]
        return rcopy(b, b, fw_s.at[min(k, 1)], fw_r.at[k], partner)

    def forwarded(k):
        b = block[k].at[1 - core]
        return rcopy(b, b, fw_s.at[min(k, 1)], fw_r.at[k], partner)

    @pl.when(core == 1)
    def _():
        pl.semaphore_wait(go, 1)

    for k in streams:
        for o in offs:
            send(k, o).start()

    @pl.when(core == 0)
    def _():
        for k in range(GO):
            gathered(k).wait_send()
        pl.semaphore_signal(go, inc=1, device_id=partner, device_id_type=MESH)

    def pass_on(k):
        gathered(k).wait_recv()
        forward(k).start()

    def arrive(c, k):
        if c == 0:
            @pl.when(core == 0)
            def _():
                pass_on(k)

        @pl.when(core != c)
        def _():
            forwarded(k).wait_recv()

    def find_gates(c):
        ids_all = meta[c].reshape(half, LANES)
        gates_all = pltpu.roll(ids_all, LANES // 2, axis=1)
        lane = lax.broadcasted_iota(jnp.int32, (half, LANES), 1)
        for e in range(n_exp):
            eid = (me * n_exp + e).astype(jnp.float32)
            g = jnp.sum(jnp.where((ids_all == eid) & (lane < top), gates_all, 0.0), axis=1, keepdims=True)
            gate[c, e] = jnp.broadcast_to(g, (half, LANES))

    def up_chunk(c, k):
        if k == 0:
            find_gates(c)
        rows[k] = gath[k, c].astype(jnp.float32).reshape(half, kw).astype(jnp.bfloat16)
        for e in range(n_exp):
            acc = jnp.dot(rows[k], up[e, pl.ds(k * kw, kw), :], preferred_element_type=jnp.float32)
            if k > 0:
                acc = z[e] + acc
            if k < KC - 1:
                z[e] = acc
            else:
                act = gelu(acc)
                h[e] = jnp.where(wide(gate[c, e], ff) > 0.0, act, 0.0).astype(jnp.bfloat16)

    def down_chunk(c, q):
        for e in range(n_exp):
            o = jnp.dot(h[e], down[e, :, pl.ds(q * qw, qw)], preferred_element_type=jnp.float32)
            o = o.astype(jnp.bfloat16).astype(jnp.float32) * wide(gate[c, e], qw)
            o = o.reshape(side, side, tok, qw)
            part[c, q] = o if e == 0 else part[c, q] + o

    def pair_out(c, qs):
        r = pl.ds(qs[0], len(qs))
        return rcopy(part.at[c, r], pair.at[r], pair_s, pair_r.at[qs[0]], partner)

    def ring_out(c, q, d):
        lane = q % 2 == 0
        src = part.at[c, q, :, d] if lane else part.at[c, q, d]
        return rcopy(src, ring.at[q, neg(d)], ring_s, ring_r.at[q], at(0, d) if lane else at(d, 0))

    def cross_out(q, d):
        lane = q % 2 == 0
        return rcopy(line.at[q, d], cross.at[q, neg(d)], cross_s, cross_r.at[q], at(d, 0) if lane else at(0, d))

    def came(ref, ss, rs):
        return rcopy(ref, ref, ss, rs, partner)

    def stage1(c, qs):
        came(pair.at[pl.ds(qs[0], len(qs))], pair_s, pair_r.at[qs[0]]).wait_recv()
        for q in qs:
            part[c, q] = part[c, q] + pair[q]
        for q in qs:
            if c == 1 and q in direct:
                for o in offs:
                    i, j = neg(o[0]), neg(o[1])
                    rcopy(part.at[c, q, o[0], o[1]], flat.at[i * side + j], flat_s, flat_r, at(*o)).start()
            else:
                for d in line_offs:
                    ring_out(c, q, d).start()

    def stage2(c, q):
        came(ring.at[q, pl.ds(1, side - 1)], ring_s, ring_r.at[q]).wait_recv()
        own = part[c, q, :, 0] if q % 2 == 0 else part[c, q, 0]
        for d in range(1, side):
            own = own + ring[q, d]
        line[q] = own
        for d in line_offs:
            cross_out(q, d).start()

    def stage3(q):
        came(cross.at[q, pl.ds(1, side - 1)], cross_s, cross_r.at[q]).wait_recv()
        t = line[q, 0]
        for d in range(1, side):
            t = t + cross[q, d]
        y_ref[:, q * qw:(q + 1) * qw] = t.astype(y_ref.dtype)

    def stage_flat(q):
        came(flat.at[pl.ds(1, chips - 1)], flat_s, flat_r).wait_recv()
        t = part[1, q, 0, 0]
        for j in range(1, chips):
            t = t + flat[j]
        y_ref[:, q * qw:(q + 1) * qw] = t.astype(y_ref.dtype)

    direct = (QC - 1,) if FLAT else ()
    rest = [q for q in range(QC) if q not in direct]

    arrive(0, 0)
    for k in range(KC):
        arrive(0, k + 1)
        up_wait(k)
        up_chunk(0, k)
    for i, qs in enumerate(BLOCKS[0]):
        @pl.when(core == 1)
        def _():
            for k in PASS[i]:
                pass_on(k)
        for q in qs:
            down_copy(q).wait()
        for q in qs:
            down_chunk(0, q)

        @pl.when(core == 1)
        def _():
            pair_out(0, qs).start()

    arrive(1, 0)
    for k in range(KC):
        arrive(1, k + 1)
        up_chunk(1, k)
        if True:
            @pl.when(core == 0)
            def _():
                stage1(0, BLOCKS[0][k])
    for i, qs in enumerate(BLOCKS[1]):
        for q in qs:
            down_chunk(1, q)

        @pl.when(core == 0)
        def _():
            pair_out(1, qs).start()
            if i >= 2:
                stage2(0, i - 2)

        @pl.when(core == 1)
        def _():
            stage1(1, qs)

    @pl.when(core == 0)
    def _():
        for q in range(2, QC):
            stage2(0, q)
        for q in range(QC):
            stage3(q)

    @pl.when(core == 1)
    def _():
        for q in rest:
            stage2(1, q)
        for q in direct:
            stage_flat(q)
        for q in rest:
            stage3(q)
        for k in range(GO):
            gathered(k).wait_send()

    for k in range(GO, KC + 1):
        gathered(k).wait_send()
    for k in streams:
        if k == 0:
            forward(k).wait_send()
    x_all = gath.at[:, core]
    rcopy(x_all, x_all, fw_s.at[1], fw_r.at[1], partner).wait_send()

    @pl.when(core == 0)
    def _():
        came(pair, pair_s, pair_r.at[0]).wait_send()
        came(ring.at[:, pl.ds(1, side - 1)], ring_s, ring_r.at[0]).wait_send()
        came(cross.at[:, pl.ds(1, side - 1)], cross_s, cross_r.at[0]).wait_send()

    @pl.when(core == 1)
    def _():
        n = len(rest)
        came(pair, pair_s, pair_r.at[0]).wait_send()
        came(ring.at[pl.ds(0, n), pl.ds(1, side - 1)], ring_s, ring_r.at[0]).wait_send()
        came(cross.at[pl.ds(0, n), pl.ds(1, side - 1)], cross_s, cross_r.at[0]).wait_send()
        if direct:
            came(flat.at[pl.ds(1, chips - 1)], flat_s, flat_r).wait_send()


def solution(mesh):
    group = mesh.shape['ep']
    side = math.isqrt(group // 2)
    token_spec = P(('dp', 'ep'), None)
    expert_spec = P('ep', None, None)

    def local_layer(x_loc, ids_loc, gates_loc, w_up, w_down):
        tok, dim = x_loc.shape
        n_exp, _, ff = w_up.shape
        half = tok * group // 2
        qw = dim // QC
        f32, bf16 = jnp.float32, jnp.bfloat16
        dma = pltpu.SemaphoreType.DMA
        scratch = [
            pltpu.VMEM(w_up.shape, bf16),
            pltpu.VMEM(w_down.shape, bf16),
            pltpu.VMEM((KC, 2, side * side, tok, dim // KC), bf16),
            pltpu.VMEM((2, side * side, tok, LANES), f32),
            pltpu.VMEM(ids_loc.shape, jnp.int32),
            pltpu.VMEM(gates_loc.shape, f32),
            pltpu.VMEM((KC, half, dim // KC), bf16),
            pltpu.VMEM((n_exp, half, ff), f32),
            pltpu.VMEM((n_exp, half, ff), bf16),
            pltpu.VMEM((2, n_exp, half, LANES), f32),
            pltpu.VMEM((2, QC, side, side, tok, qw), f32),
            pltpu.VMEM((QC, side, side, tok, qw), f32),
            pltpu.VMEM((QC, side, side, tok, qw), f32),
            pltpu.VMEM((QC, side, tok, qw), f32),
            pltpu.VMEM((QC, side, tok, qw), f32),
            pltpu.VMEM((side * side, tok, qw), f32),
            dma((3,)), dma, dma((QC,)), pltpu.SemaphoreType.REGULAR,
            dma((KC + 1,)), dma((KC + 1,)), dma((2,)), dma((KC + 1,)),
            dma, dma((QC,)), dma, dma((QC,)), dma, dma((QC,)), dma, dma,
        ]
        return pl.pallas_call(
            functools.partial(moe_kernel, side),
            out_shape=pltpu.VMEM((tok, dim), bf16),
            in_specs=[pl.BlockSpec(memory_space=pl.ANY)] * 5,
            out_specs=pl.BlockSpec(memory_space=pltpu.VMEM),
            scratch_shapes=scratch,
            compiler_params=pltpu.CompilerParams(collective_id=0, has_side_effects=True, vmem_limit_bytes=60 * 1024 * 1024),
        )(x_loc, ids_loc, gates_loc, w_up, w_down)

    return jax.shard_map(local_layer, mesh=mesh, in_specs=(token_spec, token_spec, token_spec, expert_spec, expert_spec), out_specs=token_spec, check_vma=False)
```
